32 devices in a mesh: groups: 2 (over y), tm: 4 (over z), chan: 4 (over x, core).
Axes of the slice: x: 2, y: 2, z: 4, core: 2. Of those that a mesh axis runs over, the one named last changes fastest.
Arguments:
- vis: bfloat16 [8, 128, 2, 128], P(('groups', 'chan'), 'tm'), parts along dimension 0, may hold values from -6 to 6
- row_weight: bfloat16 [8, 128, 128, 128], P(('groups', 'chan'), 'tm'), parts along dimension 0, may hold values from -4 to 4
- col_weight: bfloat16 [8, 128, 128, 256], P(('groups', 'chan'), 'tm'), parts along dimension 0, may hold values from -0.5 to 0.5
- w_bin: int32 [8, 128, 1], P(('groups', 'chan'), 'tm'), parts along dimension 0, may hold values from 0 to 3; in each aligned block of 32 rows (0 to 31, 32 to 63, ..., all dimensions but the last counted through in order) at most 16 rows name the same one
- tile_col: int32 [8, 128], P(('groups', 'chan'), 'tm'), parts along dimension 0, may hold values from 0 to 15
- w_kernel: bfloat16 [8, 512, 512], P(('groups', 'tm')), parts along dimension 0, may hold values from -0.25 to 0.25
Outputs:
- grid: float32 [8, 128, 16, 512], P(('groups', 'tm'), 'chan'), parts along dimension 0
The draws below stay inside these ranges and needn't reach their ends.
There are 2 independent parts, one for each index of `groups`. The reference program is written for one: setup_inputs(seed, part) draws one part's arguments, and reference() takes and returns one part's arrays. A program takes and returns all parts, laid end to end along the dimension named above; each array names one. Nothing has to cross between parts.
Inputs may be any that keep to these rules, and one draw needn't show every extreme that they name: `w_bin`: within the blocks of one device (aligned blocks of 32 along the channel-group and block dimensions taken together), no w-plane is named more than 16 times, a bound that some block reaches.
All inputs are finite; a program needn't handle non-finite values.
Results may differ from the reference program's by a relative error of at most 0.0041.
Values may be sent and summed in bfloat16 or wider, within the bound.
No kernel may reach another device: no remote copies, remote signals or barrier semaphores. Data moves between devices by JAX's collectives and lax.ppermute only.
A program may use at most 128 MiB of HBM per device.

```python
import math
import jax
import jax.numpy as jnp
import numpy as np
from jax import lax

VIS = 128
KROWS = 128
QW = 256
BLK_DEV = 32
TC = 16
NW = 4
BLOCKS = 128
CHANS = 4
CAP = 16


def touch_ends(drawn, stream_key, smallest, top_value):
    spot = [jax.random.randint(jax.random.fold_in(stream_key, axis), (), 0, length) for axis, length in enumerate(drawn.shape)]
    longest = drawn.shape.index(max(drawn.shape))
    next_to = spot[:longest] + [(spot[longest] + 1) % drawn.shape[longest]] + spot[longest + 1:]
    return drawn.at[tuple(spot)].set(smallest).at[tuple(next_to)].set(top_value)


def steps_of(own_key, extent, cuts, low, high):
    def one(dim, blocks):
        steps = jax.random.uniform(jax.random.fold_in(jax.random.fold_in(own_key, 6), dim), (blocks,), jnp.float32, low / len(cuts), high / len(cuts))
        return jnp.repeat(jnp.exp(steps), extent[dim] // blocks).reshape((-1,) + (1,) * (len(extent) - dim - 1))

    level = one(*cuts[0])
    for cut in cuts[1:]:
        level = level * one(*cut)
    return level


def deal_out(rng, own, number, rows, count, top, most, skew):
    ranking = jax.random.permutation(rng, count)
    crowded, ordinary = portions_of(count, rows * top, most, skew, True), portions_of(count, rows * top, most, skew, False)
    places = jnp.arange(count)

    def named(lengths, turn):
        used = int((lengths > 0).sum())
        fixed = max(1, used // 4)
        moved = fixed + (places - fixed + turn * (used - fixed)) % max(1, count - fixed)
        return jnp.zeros((count,), jnp.int32).at[ranking[jnp.where(places < fixed, places, moved)]].set(jnp.asarray(lengths, jnp.int32))

    lengths = jnp.where(number % 4 == 0, named(crowded, number // 4), named(ordinary, number - number // 4 - 1))
    mixed = jax.random.permutation(jax.random.fold_in(own, 3), count)
    source_of, taker = mixed[0:count // 2 * 2:2], mixed[1:count // 2 * 2:2]
    margin = jnp.minimum(lengths[source_of] - 1, most - lengths[taker]) // 2
    margin = jnp.where((source_of == ranking[0]) | (taker == ranking[0]) | (lengths[taker] == 0), 0, jnp.maximum(margin, 0))
    moved = jax.random.randint(jax.random.fold_in(own, 4), (count // 2,), 0, 1 << 20) % (margin + 1)
    lengths = lengths.at[source_of].add(-moved).at[taker].add(moved)
    items = jnp.searchsorted(jnp.cumsum(lengths), jnp.arange(rows * top), side="right").astype(jnp.int32)
    table = items.reshape(top, rows).T
    table = table[jax.random.permutation(jax.random.fold_in(own, 1), rows)]
    turn = jax.random.randint(jax.random.fold_in(own, 2), (rows, 1), 0, top)
    return jnp.take_along_axis(table, (jnp.arange(top)[None, :] + turn) % top, axis=1)


def portions_of(number_of, total, most, skew, full):
    weights = [(1 << 20) // math.isqrt(grade ** skew) + 1 for grade in range(1, number_of + 1)]
    largest = most if full else min(most, max(-(-total // number_of), total * weights[0] // sum(weights)))
    least = 1 if total - largest >= number_of - 1 else 0
    given, spare = [largest] + [least] * (number_of - 1), total - largest - least * (number_of - 1)
    while spare > 0:
        candidates = [i for i in range(1, number_of) if given[i] < largest] or [i for i in range(1, number_of) if given[i] < most]
        whole, left = sum([weights[i] for i in candidates]), spare
        for i in candidates:
            extra = min(most - given[i], max(1, left * weights[i] // whole), spare)
            given[i] = given[i] + extra
            spare = spare - extra
    return np.array(given)


def gaussian(own_key, shape, width, reach, shards=(), held_as=jnp.bfloat16):
    loudness = steps_of(own_key, shape, shards, -0.22, 0.18) if shards else 1.0
    array = jax.random.normal(own_key, shape, jnp.float32) * width * loudness
    return jnp.minimum(jnp.maximum(array, -reach), reach).astype(held_as)


def setup_inputs(seed: int = 0, part: int = 0) -> dict:
    seeds = jax.random.split(jax.random.key(seed), 7)
    part_keys = jax.random.split(jax.random.fold_in(seeds[6], part), 7)
    vis = gaussian(part_keys[0], (CHANS, BLOCKS, 2, VIS), 1.0, 6.0, ((0, 4), (1, 4)))
    row_weight = gaussian(part_keys[1], (CHANS, BLOCKS, KROWS, VIS), 0.25, 4.0, ((0, 4), (1, 4)))
    col_weight = gaussian(part_keys[2], (CHANS, BLOCKS, VIS, QW), VIS ** -0.5, 0.5, ((0, 4), (1, 4)))
    w_bin_keys = jax.random.split(jax.random.fold_in(part_keys[3], 1), CHANS * BLOCKS // BLK_DEV)
    w_bin_turns = jax.random.permutation(jax.random.fold_in(part_keys[3], 3), CHANS * BLOCKS // BLK_DEV)
    w_bin = jax.vmap(lambda own, number: deal_out(jax.random.fold_in(part_keys[3], 2), own, number, BLK_DEV, NW, 1, CAP, 2))(w_bin_keys, w_bin_turns).reshape((CHANS, BLOCKS, 1))
    tile_col = touch_ends(jax.random.randint(part_keys[4], (CHANS, BLOCKS), 0, TC), jax.random.fold_in(part_keys[4], 1), 0, TC - 1).astype(jnp.int32)
    w_kernel = gaussian(part_keys[5], (NW, 2 * QW, 2 * QW), (2 * QW) ** -0.5, 0.25, ((0, 4),))
    return {"vis": vis, "row_weight": row_weight, "col_weight": col_weight, "w_bin": w_bin, "tile_col": tile_col, "w_kernel": w_kernel}


def reference(vis, row_weight, col_weight, w_bin, tile_col, w_kernel):
    total_blocks = CHANS * BLOCKS
    vis_all = vis.reshape(total_blocks // BLK_DEV, BLK_DEV, 2, VIS)
    rows_all = row_weight.reshape(total_blocks // BLK_DEV, BLK_DEV, KROWS, VIS)
    cols_all = col_weight.reshape(total_blocks // BLK_DEV, BLK_DEV, VIS, QW)
    seg_all = (w_bin[:, :, 0] * TC + tile_col).astype(jnp.int32).reshape(total_blocks // BLK_DEV, BLK_DEV)

    def step(acc, group):
        vis_g, rows_g, cols_g, seg_g = group
        weighted = (rows_g.astype(jnp.float32)[:, None, :, :] * vis_g.astype(jnp.float32)[:, :, None, :]).astype(jnp.bfloat16)
        patch = jnp.einsum('ghkv,gvq->gkhq', weighted.astype(jnp.float32), cols_g.astype(jnp.float32))
        patch = patch.reshape(BLK_DEV, KROWS, 2 * QW)
        return acc.at[seg_g].add(patch), None

    start = jnp.zeros((NW * TC, KROWS, 2 * QW), jnp.float32)
    acc, _ = lax.scan(step, start, (vis_all, rows_all, cols_all, seg_all))
    pre_rounded = acc.reshape(NW, TC, KROWS, 2 * QW).astype(jnp.bfloat16)
    return jnp.einsum('wtkq,wqr->wktr', pre_rounded.astype(jnp.float32), w_kernel.astype(jnp.float32))
```

```python
import functools
import jax
import jax.numpy as jnp
from jax import lax
from jax.experimental import pallas as pl
from jax.experimental.pallas import tpu as pltpu
from jax.sharding import PartitionSpec as P

QW = 256
GC = 4096


def grid_group(total, weighted, columns, targets):
    patch = jnp.einsum("ghkv,gvq->gkhq", weighted, columns, preferred_element_type=jnp.float32)
    flat = patch.reshape(patch.shape[0], -1)
    return total.at[targets].add(flat, mode="drop")


def weigh_rows(rows, visibility):
    return (
        rows.astype(jnp.float32)[:, None, :, :] * visibility.astype(jnp.float32)[:, :, None, :]
    ).astype(jnp.bfloat16)


def raw_body(vis, row_weight, col_weight, w_bin, tile_col, w_kernel):
    planes = lax.axis_size("tm")
    count = vis.shape[1]
    rows_k = row_weight.shape[2]
    width_v = vis.shape[3]
    width_q = col_weight.shape[3]
    tile_count = GC // QW
    per_plane = 2 * count // planes
    slot_total = planes * per_plane
    turns = 4
    group_len = slot_total // turns
    bins = w_bin[0, :, 0]
    tiles = tile_col[0]
    member = (bins[:, None] == jnp.arange(planes, dtype=jnp.int32)[None, :]).astype(jnp.int32)
    before = jnp.cumsum(member, axis=0) - member
    within = jnp.sum(before * member, axis=1)
    target = bins * per_plane + within
    source = (
        jnp.full((slot_total,), count, jnp.int32).at[target].set(jnp.arange(count, dtype=jnp.int32))
    )
    filled = source < count
    picked = jnp.minimum(source, count - 1)
    slot_tile = jnp.where(filled, tiles[picked], tile_count).reshape(planes, per_plane)
    columns = jnp.take(col_weight[0], picked, axis=0).reshape(planes, per_plane, width_v, width_q)
    start = jnp.zeros((tile_count, rows_k * 2 * width_q), jnp.float32)
    rows_sent = jnp.take(row_weight[0], picked, axis=0).reshape(planes, per_plane, rows_k, width_v)
    vis_sent = jnp.take(vis[0], picked, axis=0).reshape(planes, per_plane, 2, width_v)
    got_rows, got_vis, got_columns, got_tiles = (
        lax.all_to_all(rows_sent, "tm", split_axis=0, concat_axis=0, tiled=True),
        lax.all_to_all(vis_sent, "tm", split_axis=0, concat_axis=0, tiled=True),
        lax.all_to_all(columns, "tm", split_axis=0, concat_axis=0, tiled=True),
        lax.all_to_all(slot_tile, "tm", split_axis=0, concat_axis=0, tiled=True),
    )

    def step_raw(total, group):
        rows, visibility, cols, targets = group
        return (grid_group(total, weigh_rows(rows, visibility), cols, targets), None)

    groups = (
        got_rows.reshape(turns, group_len, rows_k, width_v),
        got_vis.reshape(turns, group_len, 2, width_v),
        got_columns.reshape(turns, group_len, width_v, width_q),
        got_tiles.reshape(turns, group_len),
    )
    total, _ = lax.scan(step_raw, start, groups)
    partial_value = total.reshape(tile_count, rows_k, 2 * width_q)
    share = rows_k // lax.axis_size("chan")
    summed = lax.psum(partial_value, "chan")
    mine = lax.dynamic_slice_in_dim(summed, lax.axis_index("chan") * share, share, 1)
    rounded = mine.astype(jnp.bfloat16)
    result = jnp.einsum("tkq,qr->ktr", rounded, w_kernel[0], preferred_element_type=jnp.float32)
    return result[None]


def plane_kernel(
    tile_count, share, halves,
    meta, vis_a, rows_a, cols_a, vis_b, rows_b, cols_b,
    own, send, acc,
):
    count = vis_a.shape[0]
    width_q = cols_a.shape[2]
    plane = meta[0]
    starts = [pl.multiple_of(meta[1 + d], share) for d in range(halves)]
    base = 1 + halves
    acc[...] = jnp.zeros_like(acc)

    def one(block, which, vis, rows, cols):
        code = meta[base + which * count + block]

        @pl.when(lax.div(code, tile_count) == plane)
        def _():
            tile = lax.rem(code, tile_count)
            weights = jnp.concatenate(
                [rows[block, pl.ds(start, share), :] for start in starts], axis=0
            ).astype(jnp.float32)
            values = vis[block].astype(jnp.float32)
            weighted = jnp.concatenate(
                [weights * values[0:1, :], weights * values[1:2, :]], axis=0
            ).astype(jnp.bfloat16)
            patch = jnp.dot(weighted, cols[block], preferred_element_type=jnp.float32)
            height = halves * share
            acc[tile, :, :width_q] += patch[:height]
            acc[tile, :, width_q:] += patch[height:]

    def step(block, carry):
        one(block, 0, vis_a, rows_a, cols_a)
        one(block, 1, vis_b, rows_b, cols_b)
        return carry

    lax.fori_loop(0, count, step, 0)
    own[...] = acc[:, :share, :]
    for d in range(1, halves):
        send[d - 1] = acc[:, d * share:(d + 1) * share, :].astype(jnp.bfloat16)


def grid_plane(meta, mine, other, tile_count, share, halves):
    width = 2 * mine[2].shape[2]
    vmem = pl.BlockSpec(memory_space=pltpu.VMEM)
    return pl.pallas_call(
        functools.partial(plane_kernel, tile_count, share, halves),
        out_shape=(
            jax.ShapeDtypeStruct((tile_count, share, width), jnp.float32),
            jax.ShapeDtypeStruct((halves - 1, tile_count, share, width), jnp.bfloat16),
        ),
        in_specs=[pl.BlockSpec(memory_space=pltpu.SMEM)] + [vmem] * 6,
        out_specs=(vmem, vmem),
        scratch_shapes=[pltpu.VMEM((tile_count, halves * share, width), jnp.float32)],
        compiler_params=pltpu.CompilerParams(vmem_limit_bytes=24 << 20),
        name="grid_plane",
    )(meta, *mine, *other)


def finish_kernel(parts, own, *refs):
    received, kernel, out = refs[:parts], refs[parts], refs[parts + 1]
    total = own[...]
    for part in received:
        total = total + part[...].astype(jnp.float32)
    tiles, share, width = total.shape
    rounded = total.astype(jnp.bfloat16).reshape(tiles * share, width)
    result = jnp.dot(rounded, kernel[...], preferred_element_type=jnp.float32)
    out[...] = jnp.swapaxes(result.reshape(tiles, share, width), 0, 1)


def finish(own, received, kernel):
    tiles, share, width = own.shape
    return pl.pallas_call(
        functools.partial(finish_kernel, len(received)),
        out_shape=jax.ShapeDtypeStruct((share, tiles, width), jnp.float32),
        compiler_params=pltpu.CompilerParams(vmem_limit_bytes=16 << 20),
        name="finish",
    )(own, *received, kernel)


def swap(value, axis, bit):
    size = lax.axis_size(axis)
    return lax.ppermute(value, axis, [(i, i ^ bit) for i in range(size)])


def dense_body(vis, row_weight, col_weight, w_bin, tile_col, w_kernel):
    planes, chans = lax.axis_size("tm"), lax.axis_size("chan")
    rows_k = row_weight.shape[2]
    tile_count = GC // QW
    share, halves = rows_k // chans, chans // 2
    me, time = lax.axis_index("chan"), lax.axis_index("tm")
    code = w_bin[0, :, 0] * tile_count + tile_col[0]
    mine = (vis[0], row_weight[0], col_weight[0])
    other = tuple(swap(value, "chan", 1) for value in mine)
    codes = jnp.concatenate([code, swap(code, "chan", 1)])
    starts = jnp.stack([(me ^ (2 * d)) * share for d in range(halves)])

    parts = {}
    for r in reversed(range(planes)):
        meta = jnp.concatenate([(time ^ r)[None], starts, codes]).astype(jnp.int32)
        own, send = grid_plane(meta, mine, other, tile_count, share, halves)
        pieces = {0: own} | {d: send[d - 1] for d in range(1, halves)}
        bit = halves // 2
        while bit:
            for d in range(bit):
                got = swap(pieces[d + bit].astype(jnp.bfloat16), "chan", 2 * bit)
                pieces[d] = pieces[d].astype(jnp.float32) + got.astype(jnp.float32)
            bit //= 2
        parts[r] = [pieces[0]]

    def added(values):
        total = values[0].astype(jnp.float32)
        for value in values[1:]:
            total = total + value.astype(jnp.float32)
        return total

    bit = 1
    while bit < planes:
        for r in reversed(range(bit, planes, 2 * bit)):
            parts[r - bit].append(swap(added(parts[r]).astype(jnp.bfloat16), "tm", bit))
        bit *= 2
    return finish(parts[0][0], parts[0][1:], w_kernel[0])[None]


def body(vis, row_weight, col_weight, w_bin, tile_col, w_kernel):
    planes, chans = lax.axis_size("tm"), lax.axis_size("chan")
    count, _, width_v = vis.shape[1:]
    rows_k, width_q = row_weight.shape[2], col_weight.shape[3]
    dense = planes * (GC // QW) * rows_k * 2 * width_q
    raw = 2 * count * width_v * (rows_k + width_q + 2)
    powers = planes & (planes - 1) == 0 and chans & (chans - 1) == 0 and chans > 1
    chosen = dense_body if powers and dense <= 2 * raw else raw_body
    return chosen(vis, row_weight, col_weight, w_bin, tile_col, w_kernel)


def solution(mesh):
    in_specs = (
        P(("groups", "chan"), "tm", None, None),
        P(("groups", "chan"), "tm", None, None),
        P(("groups", "chan"), "tm", None, None),
        P(("groups", "chan"), "tm", None),
        P(("groups", "chan"), "tm"),
        P(("groups", "tm"), None, None),
    )
    out_specs = P(("groups", "tm"), "chan", None, None)
    return jax.shard_map(body, mesh=mesh, in_specs=in_specs, out_specs=out_specs, check_vma=False)
```

```python
import functools
import jax
import jax.numpy as jnp
from jax import lax
from jax.experimental import pallas as pl
from jax.experimental.pallas import tpu as pltpu
from jax.sharding import PartitionSpec as P

QW = 256
GC = 4096
TOGETHER = 4


def grid_group(total, weighted, columns, targets):
    patch = jnp.einsum("ghkv,gvq->gkhq", weighted, columns, preferred_element_type=jnp.float32)
    flat = patch.reshape(patch.shape[0], -1)
    return total.at[targets].add(flat, mode="drop")


def weigh_rows(rows, visibility):
    return (
        rows.astype(jnp.float32)[:, None, :, :] * visibility.astype(jnp.float32)[:, :, None, :]
    ).astype(jnp.bfloat16)


def raw_body(vis, row_weight, col_weight, w_bin, tile_col, w_kernel):
    planes = lax.axis_size("tm")
    count = vis.shape[1]
    rows_k = row_weight.shape[2]
    width_v = vis.shape[3]
    width_q = col_weight.shape[3]
    tile_count = GC // QW
    per_plane = 2 * count // planes
    slot_total = planes * per_plane
    turns = 4
    group_len = slot_total // turns
    bins = w_bin[0, :, 0]
    tiles = tile_col[0]
    member = (bins[:, None] == jnp.arange(planes, dtype=jnp.int32)[None, :]).astype(jnp.int32)
    before = jnp.cumsum(member, axis=0) - member
    within = jnp.sum(before * member, axis=1)
    target = bins * per_plane + within
    source = (
        jnp.full((slot_total,), count, jnp.int32).at[target].set(jnp.arange(count, dtype=jnp.int32))
    )
    filled = source < count
    picked = jnp.minimum(source, count - 1)
    slot_tile = jnp.where(filled, tiles[picked], tile_count).reshape(planes, per_plane)
    columns = jnp.take(col_weight[0], picked, axis=0).reshape(planes, per_plane, width_v, width_q)
    start = jnp.zeros((tile_count, rows_k * 2 * width_q), jnp.float32)
    rows_sent = jnp.take(row_weight[0], picked, axis=0).reshape(planes, per_plane, rows_k, width_v)
    vis_sent = jnp.take(vis[0], picked, axis=0).reshape(planes, per_plane, 2, width_v)
    got_rows, got_vis, got_columns, got_tiles = (
        lax.all_to_all(rows_sent, "tm", split_axis=0, concat_axis=0, tiled=True),
        lax.all_to_all(vis_sent, "tm", split_axis=0, concat_axis=0, tiled=True),
        lax.all_to_all(columns, "tm", split_axis=0, concat_axis=0, tiled=True),
        lax.all_to_all(slot_tile, "tm", split_axis=0, concat_axis=0, tiled=True),
    )

    def step_raw(total, group):
        rows, visibility, cols, targets = group
        return (grid_group(total, weigh_rows(rows, visibility), cols, targets), None)

    groups = (
        got_rows.reshape(turns, group_len, rows_k, width_v),
        got_vis.reshape(turns, group_len, 2, width_v),
        got_columns.reshape(turns, group_len, width_v, width_q),
        got_tiles.reshape(turns, group_len),
    )
    total, _ = lax.scan(step_raw, start, groups)
    partial_value = total.reshape(tile_count, rows_k, 2 * width_q)
    share = rows_k // lax.axis_size("chan")
    summed = lax.psum(partial_value, "chan")
    mine = lax.dynamic_slice_in_dim(summed, lax.axis_index("chan") * share, share, 1)
    rounded = mine.astype(jnp.bfloat16)
    result = jnp.einsum("tkq,qr->ktr", rounded, w_kernel[0], preferred_element_type=jnp.float32)
    return result[None]


def plane_kernel(tile_count, kinds, halves, share, begun, parts, meta, *refs):
    sources = [refs[3 * i: 3 * i + 3] for i in range(len(kinds))]
    refs = refs[3 * len(kinds):]
    first, refs = (refs[0], refs[1:]) if begun else (None, refs)
    outputs, (acc, vis_at, rows_at, cols_at, block_at, tile_at, sems) = refs[:-7], refs[-7:]
    count, width_q = sources[0][2].shape[0], sources[0][2].shape[2]
    base, half, core = meta[0], meta[1], meta[2]

    def copies(vis, rows, cols, block, slot):
        pairs = [(cols.at[block], cols_at.at[slot]), (vis.at[block], vis_at.at[slot])]
        for d in range(halves):
            pairs.append((rows.at[block, half ^ d, core], rows_at.at[slot, d]))
        return [
            pltpu.make_async_copy(src, dst, sems.at[slot, i]) for i, (src, dst) in enumerate(pairs)
        ]

    def look(source, block, filled):
        tile = meta[3 + source * count + block] - base
        hit = (tile >= 0) & (tile < tile_count)

        @pl.when(hit)
        def _():
            block_at[source, filled] = block
            tile_at[source, filled] = tile
            if kinds[source] == "hbm":
                for copy in copies(*sources[source], block, filled):
                    copy.start()

        return filled + hit.astype(jnp.int32)

    filled = [
        lax.fori_loop(0, count, functools.partial(look, source), jnp.int32(0), unroll=4)
        for source in range(len(kinds))
    ]
    acc[:tile_count] = first[...] if begun else jnp.zeros_like(acc[:tile_count])

    def patch(source, slot):
        if kinds[source] == "hbm":
            values, cols = vis_at[slot], cols_at[slot]
            weights = rows_at[slot].reshape(halves * share, rows_at.shape[3])
        else:
            vis, rows, columns = sources[source]
            block = block_at[source, slot]
            values, cols = vis[block], columns[block]
            which = core if rows.shape[2] > 1 else 0
            weights = jnp.concatenate([rows[block, half ^ d, which] for d in range(halves)], axis=0)
        weighted = jnp.concatenate([weights * values[0:1, :], weights * values[1:2, :]], axis=0)
        return jnp.dot(weighted, cols, preferred_element_type=jnp.float32)

    def add(tile, value):
        height = halves * share
        acc[tile, :, :width_q] += value[:height]
        acc[tile, :, width_q:] += value[height:]

    def step(source, i, carry):
        slots = [TOGETHER * i + j for j in range(TOGETHER)]
        for slot in slots:
            if kinds[source] == "hbm":

                @pl.when(slot < filled[source])
                def _():
                    for copy in copies(*sources[source], 0, slot):
                        copy.wait()

        if kinds[source] != "hbm":
            slots = [jnp.minimum(slot, filled[source] - 1) for slot in slots]
        values = [patch(source, slot) for slot in slots]
        for j, (slot, value) in enumerate(zip(slots, values)):
            valid = TOGETHER * i + j < filled[source]
            add(jnp.where(valid, tile_at[source, slot], tile_count), value)
        return carry

    for source in sorted(range(len(kinds)), key=lambda source: kinds[source] == "hbm"):
        groups = lax.div(filled[source] + TOGETHER - 1, TOGETHER)
        lax.fori_loop(0, groups, functools.partial(step, source), 0)
    if not parts:
        outputs[0][...] = acc[:tile_count]
    outputs = list(outputs)
    for low, high, dtypes in parts:
        for d in range(len(dtypes)):
            rows = acc[low:high, d * share:(d + 1) * share, :]
            out = outputs.pop(0)
            out[...] = rows.astype(out.dtype)


def grid_plane(meta, sources, kinds, halves, tile_count, cap, parts, first=None):
    count, width_v, width_q = sources[0][2].shape
    share = sources[0][1].shape[3]
    width = 2 * width_q
    vmem = pl.BlockSpec(memory_space=pltpu.VMEM)
    hbm = pl.BlockSpec(memory_space=pltpu.HBM)
    slots = -(-cap // TOGETHER) * TOGETHER
    specs, operands = [pl.BlockSpec(memory_space=pltpu.SMEM)], [meta]
    for source, kind in zip(sources, kinds):
        for value in source:
            specs.append(hbm if kind == "hbm" else vmem)
            operands.append(
                pltpu.with_memory_space_constraint(value, pltpu.HBM) if kind == "hbm" else value
            )
    if first is not None:
        specs.append(vmem)
        operands.append(first)
    wide = jnp.float32
    shapes = (jax.ShapeDtypeStruct((tile_count, halves * share, width), wide),)
    if parts:
        shapes = tuple(
            jax.ShapeDtypeStruct((high - low, share, width), dtype)
            for low, high, dtypes in parts
            for dtype in dtypes
        )
    flops = 4 * len(sources) * (count // 4) * halves * share * width_v * width_q
    return pl.pallas_call(
        functools.partial(plane_kernel, tile_count, kinds, halves, share, first is not None, parts),
        out_shape=shapes,
        in_specs=specs,
        out_specs=(vmem,) * len(shapes),
        scratch_shapes=[
            pltpu.VMEM((tile_count + 1, halves * share, width), wide),
            pltpu.VMEM((slots, 2, width_v), jnp.bfloat16),
            pltpu.VMEM((slots, halves, share, width_v), jnp.bfloat16),
            pltpu.VMEM((slots, width_v, width_q), jnp.bfloat16),
            pltpu.SMEM((len(sources), slots), jnp.int32),
            pltpu.SMEM((len(sources), slots), jnp.int32),
            pltpu.SemaphoreType.DMA((slots, 2 + halves)),
        ],
        compiler_params=pltpu.CompilerParams(vmem_limit_bytes=8 << 20),
        cost_estimate=pl.CostEstimate(
            flops=flops * 8, transcendentals=0, bytes_accessed=4 << 20
        ),
        name="grid_plane",
    )(*operands)


def added(*values):
    total = values[0].astype(jnp.float32)
    for value in values[1:]:
        total = total + value.astype(jnp.float32)
    return total


def finish_kernel(parts, *refs):
    kernel, out = refs[parts], refs[-1]
    total = added(*[ref[...] for ref in refs[:parts]])
    tiles, share, width = total.shape
    rounded = total.astype(jnp.bfloat16).reshape(tiles * share, width)
    result = jnp.dot(rounded, kernel[...], preferred_element_type=jnp.float32)
    out[...] = jnp.swapaxes(result.reshape(tiles, share, width), 0, 1)


def finish(pieces, kernel, part, tile_count, rest=None):
    tiles, share, width = pieces[0].shape
    vmem = pl.BlockSpec(memory_space=pltpu.VMEM)
    more = () if rest is None else (rest,)
    return pl.pallas_call(
        functools.partial(finish_kernel, len(pieces)),
        out_shape=jax.ShapeDtypeStruct((share, tile_count, width), jnp.float32),
        grid=(1,),
        in_specs=[vmem] * (len(pieces) + 1) + [pl.BlockSpec(memory_space=pl.ANY)] * len(more),
        out_specs=pl.BlockSpec((share, tiles, width), lambda i: (0, part, 0)),
        input_output_aliases={len(pieces) + 1: 0} if more else {},
        compiler_params=pltpu.CompilerParams(vmem_limit_bytes=8 << 20),
        name="finish",
    )(*pieces, kernel, *more)


def swap(value, axis, bit):
    size = lax.axis_size(axis)
    return lax.ppermute(value, axis, [(i, i ^ bit) for i in range(size)])


def added(*values):
    total = values[0].astype(jnp.float32)
    for value in values[1:]:
        total = total + value.astype(jnp.float32)
    return total


def dense_body(vis, row_weight, col_weight, w_bin, tile_col, w_kernel):
    planes, chans = lax.axis_size("tm"), lax.axis_size("chan")
    count, rows_k, width_v = row_weight.shape[1:]
    tile_count = GC // QW
    share, halves = rows_k // chans, chans // 2
    cap = 2 * count // planes
    me, time = lax.axis_index("chan"), lax.axis_index("tm")
    half, core = me // 2, me % 2
    code = w_bin[0, :, 0] * tile_count + tile_col[0]
    rows = row_weight[0].reshape(count, halves, 2, share, width_v)
    mine = (vis[0], rows, col_weight[0])
    given = lax.dynamic_slice_in_dim(rows, core ^ 1, 1, 2)
    other = tuple(swap(value, "chan", 1) for value in (vis[0], given, col_weight[0]))
    code_b = swap(code, "chan", 1)
    low = jnp.bfloat16

    def grid(r, tiles, sources, parts, first=None):
        begin = (time ^ r) * tile_count + tiles.start
        codes = [code if source is mine[0] else code_b for source, _ in sources]
        meta = jnp.concatenate([jnp.stack([begin, half, core]), *codes]).astype(jnp.int32)
        return grid_plane(
            meta, [source for source, _ in sources], [kind for _, kind in sources],
            halves, len(tiles), cap, parts, first,
        )

    mine, other = (mine, "hbm"), (other, "vmem")
    every, middle = range(tile_count), tile_count // 2
    wide = jnp.float32
    half_a, half_b = (0, middle, (wide, low)), (middle, tile_count, (wide, low))
    (begun,) = grid(3, every[:middle], [mine], ())
    begun = pltpu.with_memory_space_constraint(begun, pltpu.VMEM)
    o3a, s3a = grid(3, every[:middle], [other], (half_a,), begun)
    both = [mine, other]
    o2a, s2a, o2b, s2b = grid(2, every, both, (half_a, half_b))
    o3b, s3b = grid(3, every[middle:], both, (half_a,))
    o1a, s1a, o1b, s1b = grid(1, every, both, (half_a, half_b))
    o0a, s0a, o0b, s0b = grid(0, every, both, (half_a, half_b))

    def give(*values):
        return added(*values).astype(low)

    x3a, x3b = swap(s3a, "chan", 2), swap(s3b, "chan", 2)
    x2a, x2b = swap(s2a, "chan", 2), swap(s2b, "chan", 2)
    x1a, x1b = swap(s1a, "chan", 2), swap(s1b, "chan", 2)
    x0a, x0b = swap(s0a, "chan", 2), swap(s0b, "chan", 2)
    z3a = swap(give(o3a, x3a), "tm", 1)
    z3b = swap(give(o3b, x3b), "tm", 1)
    z2a = swap(give(o2a, x2a, z3a), "tm", 2)
    z2b = swap(give(o2b, x2b, z3b), "tm", 2)
    z1a = swap(give(o1a, x1a), "tm", 1)
    z1b = swap(give(o1b, x1b), "tm", 1)
    out = finish((o0a, x0a, z1a, z2a), w_kernel[0], 0, tile_count)
    out = finish((o0b, x0b, z1b, z2b), w_kernel[0], 1, tile_count, out)
    return out[None]


def body(vis, row_weight, col_weight, w_bin, tile_col, w_kernel):
    planes, chans = lax.axis_size("tm"), lax.axis_size("chan")
    count, _, width_v = vis.shape[1:]
    rows_k, width_q = row_weight.shape[2], col_weight.shape[3]
    dense = planes * (GC // QW) * rows_k * 2 * width_q
    raw = 2 * count * width_v * (rows_k + width_q + 2)
    fits = planes == 4 and chans == 4 and dense <= 2 * raw
    chosen = dense_body if fits else raw_body
    return chosen(vis, row_weight, col_weight, w_bin, tile_col, w_kernel)


def solution(mesh):
    in_specs = (
        P(("groups", "chan"), "tm", None, None),
        P(("groups", "chan"), "tm", None, None),
        P(("groups", "chan"), "tm", None, None),
        P(("groups", "chan"), "tm", None),
        P(("groups", "chan"), "tm"),
        P(("groups", "tm"), None, None),
    )
    out_specs = P(("groups", "tm"), "chan", None, None)
    return jax.shard_map(body, mesh=mesh, in_specs=in_specs, out_specs=out_specs, check_vma=False)
```

```python
import functools
import jax
import jax.numpy as jnp
from jax import lax
from jax.experimental import pallas as pl
from jax.experimental.pallas import tpu as pltpu
from jax.sharding import PartitionSpec as P

QW = 256
GC = 4096
TOGETHER = 4


def grid_group(total, weighted, columns, targets):
    patch = jnp.einsum("ghkv,gvq->gkhq", weighted, columns, preferred_element_type=jnp.float32)
    flat = patch.reshape(patch.shape[0], -1)
    return total.at[targets].add(flat, mode="drop")


def weigh_rows(rows, visibility):
    return (
        rows.astype(jnp.float32)[:, None, :, :] * visibility.astype(jnp.float32)[:, :, None, :]
    ).astype(jnp.bfloat16)


def raw_body(vis, row_weight, col_weight, w_bin, tile_col, w_kernel):
    planes = lax.axis_size("tm")
    count = vis.shape[1]
    rows_k = row_weight.shape[2]
    width_v = vis.shape[3]
    width_q = col_weight.shape[3]
    tile_count = GC // QW
    per_plane = 2 * count // planes
    slot_total = planes * per_plane
    turns = 4
    group_len = slot_total // turns
    bins = w_bin[0, :, 0]
    tiles = tile_col[0]
    member = (bins[:, None] == jnp.arange(planes, dtype=jnp.int32)[None, :]).astype(jnp.int32)
    before = jnp.cumsum(member, axis=0) - member
    within = jnp.sum(before * member, axis=1)
    target = bins * per_plane + within
    source = (
        jnp.full((slot_total,), count, jnp.int32).at[target].set(jnp.arange(count, dtype=jnp.int32))
    )
    filled = source < count
    picked = jnp.minimum(source, count - 1)
    slot_tile = jnp.where(filled, tiles[picked], tile_count).reshape(planes, per_plane)
    columns = jnp.take(col_weight[0], picked, axis=0).reshape(planes, per_plane, width_v, width_q)
    start = jnp.zeros((tile_count, rows_k * 2 * width_q), jnp.float32)
    rows_sent = jnp.take(row_weight[0], picked, axis=0).reshape(planes, per_plane, rows_k, width_v)
    vis_sent = jnp.take(vis[0], picked, axis=0).reshape(planes, per_plane, 2, width_v)
    got_rows, got_vis, got_columns, got_tiles = (
        lax.all_to_all(rows_sent, "tm", split_axis=0, concat_axis=0, tiled=True),
        lax.all_to_all(vis_sent, "tm", split_axis=0, concat_axis=0, tiled=True),
        lax.all_to_all(columns, "tm", split_axis=0, concat_axis=0, tiled=True),
        lax.all_to_all(slot_tile, "tm", split_axis=0, concat_axis=0, tiled=True),
    )

    def step_raw(total, group):
        rows, visibility, cols, targets = group
        return (grid_group(total, weigh_rows(rows, visibility), cols, targets), None)

    groups = (
        got_rows.reshape(turns, group_len, rows_k, width_v),
        got_vis.reshape(turns, group_len, 2, width_v),
        got_columns.reshape(turns, group_len, width_v, width_q),
        got_tiles.reshape(turns, group_len),
    )
    total, _ = lax.scan(step_raw, start, groups)
    partial_value = total.reshape(tile_count, rows_k, 2 * width_q)
    share = rows_k // lax.axis_size("chan")
    summed = lax.psum(partial_value, "chan")
    mine = lax.dynamic_slice_in_dim(summed, lax.axis_index("chan") * share, share, 1)
    rounded = mine.astype(jnp.bfloat16)
    result = jnp.einsum("tkq,qr->ktr", rounded, w_kernel[0], preferred_element_type=jnp.float32)
    return result[None]


def plane_kernel(lengths, kinds, halves, share, parts, meta, *refs):
    sources = [refs[3 * i: 3 * i + 3] for i in range(len(kinds))]
    refs = refs[3 * len(kinds):]
    tile_count, ranges = sum(lengths), len(lengths)
    outputs, (acc, vis_at, rows_at, cols_at, block_at, tile_at, sems) = refs[:-7], refs[-7:]
    count, width_q = sources[0][2].shape[0], sources[0][2].shape[2]
    half, core = meta[ranges], meta[ranges + 1]

    def copies(vis, rows, cols, block, slot):
        pairs = [(cols.at[block], cols_at.at[slot]), (vis.at[block], vis_at.at[slot])]
        for d in range(halves):
            pairs.append((rows.at[block, half ^ d, core], rows_at.at[slot, d]))
        return [
            pltpu.make_async_copy(src, dst, sems.at[slot, i]) for i, (src, dst) in enumerate(pairs)
        ]

    def look(source, block, filled):
        code = meta[ranges + 2 + source * count + block]
        hit, tile, before = False, 0, 0
        for i, length in enumerate(lengths):
            inside = (code >= meta[i]) & (code < meta[i] + length)
            tile = jnp.where(inside, code - meta[i] + before, tile)
            hit, before = inside | hit, before + length

        @pl.when(hit)
        def _():
            block_at[source, filled] = block
            tile_at[source, filled] = tile
            if kinds[source] == "hbm":
                for copy in copies(*sources[source], block, filled):
                    copy.start()

        return filled + hit.astype(jnp.int32)

    filled = [
        lax.fori_loop(0, count, functools.partial(look, source), jnp.int32(0), unroll=True)
        for source in range(len(kinds))
    ]
    acc[:tile_count] = jnp.zeros_like(acc[:tile_count])

    def patch(source, slot):
        if kinds[source] == "hbm":
            values, cols = vis_at[slot], cols_at[slot]
            weights = rows_at[slot].reshape(halves * share, rows_at.shape[3])
        else:
            vis, rows, columns = sources[source]
            block = block_at[source, slot]
            values, cols = vis[block], columns[block]
            which = core if rows.shape[2] > 1 else 0
            weights = jnp.concatenate([rows[block, half ^ d, which] for d in range(halves)], axis=0)
        weighted = jnp.concatenate([weights * values[0:1, :], weights * values[1:2, :]], axis=0)
        return jnp.dot(weighted, cols, preferred_element_type=jnp.float32)

    def add(tile, value):
        height = halves * share
        acc[tile, :, :width_q] += value[:height]
        acc[tile, :, width_q:] += value[height:]

    def step(source, i, carry):
        slots = [TOGETHER * i + j for j in range(TOGETHER)]
        for slot in slots:
            if kinds[source] == "hbm":

                @pl.when(slot < filled[source])
                def _():
                    for copy in copies(*sources[source], 0, slot):
                        copy.wait()

        if kinds[source] != "hbm":
            slots = [jnp.minimum(slot, filled[source] - 1) for slot in slots]
        values = [patch(source, slot) for slot in slots]
        for j, (slot, value) in enumerate(zip(slots, values)):
            valid = TOGETHER * i + j < filled[source]
            add(jnp.where(valid, tile_at[source, slot], tile_count), value)
        return carry

    for source in sorted(range(len(kinds)), key=lambda source: kinds[source] == "hbm"):
        groups = lax.div(filled[source] + TOGETHER - 1, TOGETHER)
        lax.fori_loop(0, groups, functools.partial(step, source), 0)
    outputs = list(outputs)
    for low, high, dtypes in parts:
        for d in range(len(dtypes)):
            rows = acc[low:high, d * share:(d + 1) * share, :]
            out = outputs.pop(0)
            out[...] = rows.astype(out.dtype)


def grid_plane(meta, sources, kinds, halves, lengths, cap, parts):
    count, width_v, width_q = sources[0][2].shape
    share = sources[0][1].shape[3]
    width = 2 * width_q
    vmem = pl.BlockSpec(memory_space=pltpu.VMEM)
    hbm = pl.BlockSpec(memory_space=pltpu.HBM)
    slots = -(-min(count, cap * len(lengths)) // TOGETHER) * TOGETHER
    specs, operands = [pl.BlockSpec(memory_space=pltpu.SMEM)], [meta]
    for source, kind in zip(sources, kinds):
        for value in source:
            specs.append(hbm if kind == "hbm" else vmem)
            operands.append(
                pltpu.with_memory_space_constraint(value, pltpu.HBM) if kind == "hbm" else value
            )
    wide = jnp.float32
    shapes = tuple(
        jax.ShapeDtypeStruct((high - low, share, width), dtype)
        for low, high, dtypes in parts
        for dtype in dtypes
    )
    flops = 4 * len(sources) * (count // 4) * halves * share * width_v * width_q
    return pl.pallas_call(
        functools.partial(plane_kernel, lengths, kinds, halves, share, parts),
        out_shape=shapes,
        in_specs=specs,
        out_specs=(vmem,) * len(shapes),
        scratch_shapes=[
            pltpu.VMEM((sum(lengths) + 1, halves * share, width), wide),
            pltpu.VMEM((slots, 2, width_v), jnp.bfloat16),
            pltpu.VMEM((slots, halves, share, width_v), jnp.bfloat16),
            pltpu.VMEM((slots, width_v, width_q), jnp.bfloat16),
            pltpu.SMEM((len(sources), slots), jnp.int32),
            pltpu.SMEM((len(sources), slots), jnp.int32),
            pltpu.SemaphoreType.DMA((slots, 2 + halves)),
        ],
        compiler_params=pltpu.CompilerParams(vmem_limit_bytes=8 << 20),
        cost_estimate=pl.CostEstimate(
            flops=flops * 8, transcendentals=0, bytes_accessed=4 << 20
        ),
        name="grid_plane",
    )(*operands)


def added(*values):
    total = values[0].astype(jnp.float32)
    for value in values[1:]:
        total = total + value.astype(jnp.float32)
    return total


def finish_kernel(parts, *refs):
    kernel, out = refs[parts], refs[-1]
    total = added(*[ref[...] for ref in refs[:parts]])
    tiles, share, width = total.shape
    rounded = total.astype(jnp.bfloat16).reshape(tiles * share, width)
    result = jnp.dot(rounded, kernel[...], preferred_element_type=jnp.float32)
    out[...] = jnp.swapaxes(result.reshape(tiles, share, width), 0, 1)


def finish(pieces, kernel, part, tile_count, rest=None):
    tiles, share, width = pieces[0].shape
    vmem = pl.BlockSpec(memory_space=pltpu.VMEM)
    more = () if rest is None else (rest,)
    return pl.pallas_call(
        functools.partial(finish_kernel, len(pieces)),
        out_shape=jax.ShapeDtypeStruct((share, tile_count, width), jnp.float32),
        grid=(1,),
        in_specs=[vmem] * (len(pieces) + 1) + [pl.BlockSpec(memory_space=pl.ANY)] * len(more),
        out_specs=pl.BlockSpec((share, tiles, width), lambda i: (0, part, 0)),
        input_output_aliases={len(pieces) + 1: 0} if more else {},
        compiler_params=pltpu.CompilerParams(vmem_limit_bytes=8 << 20),
        name="finish",
    )(*pieces, kernel, *more)


def swap(value, axis, bit):
    size = lax.axis_size(axis)
    return lax.ppermute(value, axis, [(i, i ^ bit) for i in range(size)])


def added(*values):
    total = values[0].astype(jnp.float32)
    for value in values[1:]:
        total = total + value.astype(jnp.float32)
    return total


def dense_body(vis, row_weight, col_weight, w_bin, tile_col, w_kernel):
    planes, chans = lax.axis_size("tm"), lax.axis_size("chan")
    count, rows_k, width_v = row_weight.shape[1:]
    tile_count = GC // QW
    share, halves = rows_k // chans, chans // 2
    cap = 2 * count // planes
    me, time = lax.axis_index("chan"), lax.axis_index("tm")
    half, core = me // 2, me % 2
    code = w_bin[0, :, 0] * tile_count + tile_col[0]
    rows = row_weight[0].reshape(count, halves, 2, share, width_v)
    mine = (vis[0], rows, col_weight[0])
    given = lax.dynamic_slice_in_dim(rows, core ^ 1, 1, 2)
    other = tuple(swap(value, "chan", 1) for value in (vis[0], given, col_weight[0]))
    code_b = swap(code, "chan", 1)
    low = jnp.bfloat16

    def grid(ranges, *parts):
        begins = [(time ^ r) * tile_count + tiles.start for r, tiles in ranges]
        meta = jnp.concatenate([jnp.stack([*begins, half, core]), code, code_b]).astype(jnp.int32)
        lengths = tuple(len(tiles) for _, tiles in ranges)
        return grid_plane(meta, (mine, other), ("hbm", "vmem"), halves, lengths, cap, parts)

    middle, wide = tile_count // 2, jnp.float32
    every = range(tile_count)
    tiles_a, tiles_b = every[:middle], every[middle:]
    half_a, half_b = (0, middle, (wide, low)), (middle, tile_count, (wide, low))
    o3a, s3a, o1b, p1b = grid(
        [(3, tiles_a), (1, tiles_b)], half_a, (middle, tile_count, (low, low))
    )
    o2a, s2a, o2b, s2b = grid([(2, every)], half_a, half_b)
    o3b, s3b, o1a, s1a = grid([(3, tiles_b), (1, tiles_a)], half_a, half_b)
    o0a, s0a, o0b, p0b = grid([(0, every)], half_a, (middle, tile_count, (wide, wide)))

    def give(*values):
        return added(*values).astype(low)

    z1b, z1c = swap(o1b, "tm", 1), swap(p1b, "tm", 1)
    x3a, x3b = swap(s3a, "chan", 2), swap(s3b, "chan", 2)
    x2a, x2b = swap(s2a, "chan", 2), swap(s2b, "chan", 2)
    x1a, x0a = swap(s1a, "chan", 2), swap(s0a, "chan", 2)
    z3a = swap(give(o3a, x3a), "tm", 1)
    z3b = swap(give(o3b, x3b), "tm", 1)
    z2a = swap(give(o2a, x2a, z3a), "tm", 2)
    z2b = swap(give(o2b, x2b, z3b), "tm", 2)
    z1a = swap(give(o1a, x1a), "tm", 1)
    x0b = swap(give(p0b, z1c), "chan", 2)
    out = finish((o0a, x0a, z1a, z2a), w_kernel[0], 0, tile_count)
    out = finish((o0b, z1b, x0b, z2b), w_kernel[0], 1, tile_count, out)
    return out[None]


def body(vis, row_weight, col_weight, w_bin, tile_col, w_kernel):
    planes, chans = lax.axis_size("tm"), lax.axis_size("chan")
    count, _, width_v = vis.shape[1:]
    rows_k, width_q = row_weight.shape[2], col_weight.shape[3]
    dense = planes * (GC // QW) * rows_k * 2 * width_q
    raw = 2 * count * width_v * (rows_k + width_q + 2)
    fits = planes == 4 and chans == 4 and dense <= 2 * raw
    chosen = dense_body if fits else raw_body
    return chosen(vis, row_weight, col_weight, w_bin, tile_col, w_kernel)


def solution(mesh):
    in_specs = (
        P(("groups", "chan"), "tm", None, None),
        P(("groups", "chan"), "tm", None, None),
        P(("groups", "chan"), "tm", None, None),
        P(("groups", "chan"), "tm", None),
        P(("groups", "chan"), "tm"),
        P(("groups", "tm"), None, None),
    )
    out_specs = P(("groups", "tm"), "chan", None, None)
    return jax.shard_map(body, mesh=mesh, in_specs=in_specs, out_specs=out_specs, check_vma=False)
```

```python
import functools
import jax
import jax.numpy as jnp
from jax import lax
from jax.experimental import pallas as pl
from jax.experimental.pallas import tpu as pltpu
from jax.sharding import PartitionSpec as P

QW = 256
GC = 4096
TOGETHER = 4


def grid_group(total, weighted, columns, targets):
    patch = jnp.einsum("ghkv,gvq->gkhq", weighted, columns, preferred_element_type=jnp.float32)
    flat = patch.reshape(patch.shape[0], -1)
    return total.at[targets].add(flat, mode="drop")


def weigh_rows(rows, visibility):
    return (
        rows.astype(jnp.float32)[:, None, :, :] * visibility.astype(jnp.float32)[:, :, None, :]
    ).astype(jnp.bfloat16)


def raw_body(vis, row_weight, col_weight, w_bin, tile_col, w_kernel):
    planes = lax.axis_size("tm")
    count = vis.shape[1]
    rows_k = row_weight.shape[2]
    width_v = vis.shape[3]
    width_q = col_weight.shape[3]
    tile_count = GC // QW
    per_plane = 2 * count // planes
    slot_total = planes * per_plane
    turns = 4
    group_len = slot_total // turns
    bins = w_bin[0, :, 0]
    tiles = tile_col[0]
    member = (bins[:, None] == jnp.arange(planes, dtype=jnp.int32)[None, :]).astype(jnp.int32)
    before = jnp.cumsum(member, axis=0) - member
    within = jnp.sum(before * member, axis=1)
    target = bins * per_plane + within
    source = (
        jnp.full((slot_total,), count, jnp.int32).at[target].set(jnp.arange(count, dtype=jnp.int32))
    )
    filled = source < count
    picked = jnp.minimum(source, count - 1)
    slot_tile = jnp.where(filled, tiles[picked], tile_count).reshape(planes, per_plane)
    columns = jnp.take(col_weight[0], picked, axis=0).reshape(planes, per_plane, width_v, width_q)
    start = jnp.zeros((tile_count, rows_k * 2 * width_q), jnp.float32)
    rows_sent = jnp.take(row_weight[0], picked, axis=0).reshape(planes, per_plane, rows_k, width_v)
    vis_sent = jnp.take(vis[0], picked, axis=0).reshape(planes, per_plane, 2, width_v)
    got_rows, got_vis, got_columns, got_tiles = (
        lax.all_to_all(rows_sent, "tm", split_axis=0, concat_axis=0, tiled=True),
        lax.all_to_all(vis_sent, "tm", split_axis=0, concat_axis=0, tiled=True),
        lax.all_to_all(columns, "tm", split_axis=0, concat_axis=0, tiled=True),
        lax.all_to_all(slot_tile, "tm", split_axis=0, concat_axis=0, tiled=True),
    )

    def step_raw(total, group):
        rows, visibility, cols, targets = group
        return (grid_group(total, weigh_rows(rows, visibility), cols, targets), None)

    groups = (
        got_rows.reshape(turns, group_len, rows_k, width_v),
        got_vis.reshape(turns, group_len, 2, width_v),
        got_columns.reshape(turns, group_len, width_v, width_q),
        got_tiles.reshape(turns, group_len),
    )
    total, _ = lax.scan(step_raw, start, groups)
    partial_value = total.reshape(tile_count, rows_k, 2 * width_q)
    share = rows_k // lax.axis_size("chan")
    summed = lax.psum(partial_value, "chan")
    mine = lax.dynamic_slice_in_dim(summed, lax.axis_index("chan") * share, share, 1)
    rounded = mine.astype(jnp.bfloat16)
    result = jnp.einsum("tkq,qr->ktr", rounded, w_kernel[0], preferred_element_type=jnp.float32)
    return result[None]


def plane_kernel(tile_count, kinds, halves, share, parts, meta, *refs):
    sources = [refs[3 * i: 3 * i + 3] for i in range(len(kinds))]
    refs = refs[3 * len(kinds):]
    outputs, (acc, vis_at, rows_at, cols_at, block_at, tile_at, sems) = refs[:-7], refs[-7:]
    count, width_q = sources[0][2].shape[0], sources[0][2].shape[2]
    half, core = meta[0], meta[1]

    def copies(vis, rows, cols, block, slot):
        pairs = [(cols.at[block], cols_at.at[slot]), (vis.at[block], vis_at.at[slot])]
        for d in range(halves):
            pairs.append((rows.at[block, half ^ d, core], rows_at.at[slot, d]))
        return [
            pltpu.make_async_copy(src, dst, sems.at[slot, i]) for i, (src, dst) in enumerate(pairs)
        ]

    def look(source, block, filled):
        tile = meta[2 + source * count + block]
        hit = tile >= 0

        @pl.when(hit)
        def _():
            block_at[source, filled] = block
            tile_at[source, filled] = tile
            if kinds[source] == "hbm":
                for copy in copies(*sources[source], block, filled):
                    copy.start()

        return filled + hit.astype(jnp.int32)

    filled = [
        lax.fori_loop(0, count, functools.partial(look, source), jnp.int32(0), unroll=True)
        for source in range(len(kinds))
    ]
    acc[:tile_count] = jnp.zeros_like(acc[:tile_count])

    def patch(source, slot):
        if kinds[source] == "hbm":
            values, cols = vis_at[slot], cols_at[slot]
            weights = rows_at[slot].reshape(halves * share, rows_at.shape[3])
        else:
            vis, rows, columns = sources[source]
            block = block_at[source, slot]
            values, cols = vis[block], columns[block]
            which = core if rows.shape[2] > 1 else 0
            weights = jnp.concatenate([rows[block, half ^ d, which] for d in range(halves)], axis=0)
        weighted = jnp.concatenate([weights * values[0:1, :], weights * values[1:2, :]], axis=0)
        return jnp.dot(weighted, cols, preferred_element_type=jnp.float32)

    def add(tile, value):
        height = halves * share
        acc[tile, :, :width_q] += value[:height]
        acc[tile, :, width_q:] += value[height:]

    def step(source, i, carry):
        slots = [TOGETHER * i + j for j in range(TOGETHER)]
        for slot in slots:
            if kinds[source] == "hbm":

                @pl.when(slot < filled[source])
                def _():
                    for copy in copies(*sources[source], 0, slot):
                        copy.wait()

        if kinds[source] != "hbm":
            slots = [jnp.minimum(slot, filled[source] - 1) for slot in slots]
        values = [patch(source, slot) for slot in slots]
        for j, (slot, value) in enumerate(zip(slots, values)):
            valid = TOGETHER * i + j < filled[source]
            add(jnp.where(valid, tile_at[source, slot], tile_count), value)
        return carry

    for source in sorted(range(len(kinds)), key=lambda source: kinds[source] == "hbm"):
        groups = lax.div(filled[source] + TOGETHER - 1, TOGETHER)
        lax.fori_loop(0, groups, functools.partial(step, source), 0)
    outputs = list(outputs)
    for low, high, dtypes in parts:
        for d in range(len(dtypes)):
            rows = acc[low:high, d * share:(d + 1) * share, :]
            out = outputs.pop(0)
            out[...] = rows.astype(out.dtype)


def grid_plane(meta, sources, kinds, halves, lengths, cap, parts):
    count, width_v, width_q = sources[0][2].shape
    share = sources[0][1].shape[3]
    width = 2 * width_q
    vmem = pl.BlockSpec(memory_space=pltpu.VMEM)
    hbm = pl.BlockSpec(memory_space=pltpu.HBM)
    slots = -(-min(count, cap * len(lengths)) // TOGETHER) * TOGETHER
    specs, operands = [pl.BlockSpec(memory_space=pltpu.SMEM)], [meta]
    for source, kind in zip(sources, kinds):
        for value in source:
            specs.append(hbm if kind == "hbm" else vmem)
            operands.append(
                pltpu.with_memory_space_constraint(value, pltpu.HBM) if kind == "hbm" else value
            )
    wide = jnp.float32
    shapes = tuple(
        jax.ShapeDtypeStruct((high - low, share, width), dtype)
        for low, high, dtypes in parts
        for dtype in dtypes
    )
    flops = 4 * len(sources) * (count // 4) * halves * share * width_v * width_q
    return pl.pallas_call(
        functools.partial(plane_kernel, sum(lengths), kinds, halves, share, parts),
        out_shape=shapes,
        in_specs=specs,
        out_specs=(vmem,) * len(shapes),
        scratch_shapes=[
            pltpu.VMEM((sum(lengths) + 1, halves * share, width), wide),
            pltpu.VMEM((slots, 2, width_v), jnp.bfloat16),
            pltpu.VMEM((slots, halves, share, width_v), jnp.bfloat16),
            pltpu.VMEM((slots, width_v, width_q), jnp.bfloat16),
            pltpu.SMEM((len(sources), slots), jnp.int32),
            pltpu.SMEM((len(sources), slots), jnp.int32),
            pltpu.SemaphoreType.DMA((slots, 2 + halves)),
        ],
        compiler_params=pltpu.CompilerParams(vmem_limit_bytes=8 << 20),
        cost_estimate=pl.CostEstimate(
            flops=flops * 8, transcendentals=0, bytes_accessed=4 << 20
        ),
        name="grid_plane",
    )(*operands)


def added(*values):
    total = values[0].astype(jnp.float32)
    for value in values[1:]:
        total = total + value.astype(jnp.float32)
    return total


def finish_kernel(parts, *refs):
    kernel, out = refs[parts], refs[-1]
    total = added(*[ref[...] for ref in refs[:parts]])
    tiles, share, width = total.shape
    rounded = total.astype(jnp.bfloat16).reshape(tiles * share, width)
    result = jnp.dot(rounded, kernel[...], preferred_element_type=jnp.float32)
    out[...] = jnp.swapaxes(result.reshape(tiles, share, width), 0, 1)


def finish(pieces, kernel, part, tile_count, rest=None):
    tiles, share, width = pieces[0].shape
    vmem = pl.BlockSpec(memory_space=pltpu.VMEM)
    more = () if rest is None else (rest,)
    return pl.pallas_call(
        functools.partial(finish_kernel, len(pieces)),
        out_shape=jax.ShapeDtypeStruct((share, tile_count, width), jnp.float32),
        grid=(1,),
        in_specs=[vmem] * (len(pieces) + 1) + [pl.BlockSpec(memory_space=pl.ANY)] * len(more),
        out_specs=pl.BlockSpec((share, tiles, width), lambda i: (0, part, 0)),
        input_output_aliases={len(pieces) + 1: 0} if more else {},
        compiler_params=pltpu.CompilerParams(vmem_limit_bytes=8 << 20),
        name="finish",
    )(*pieces, kernel, *more)


def swap(value, axis, bit):
    size = lax.axis_size(axis)
    return lax.ppermute(value, axis, [(i, i ^ bit) for i in range(size)])


def added(*values):
    total = values[0].astype(jnp.float32)
    for value in values[1:]:
        total = total + value.astype(jnp.float32)
    return total


def dense_body(vis, row_weight, col_weight, w_bin, tile_col, w_kernel):
    planes, chans = lax.axis_size("tm"), lax.axis_size("chan")
    count, rows_k, width_v = row_weight.shape[1:]
    tile_count = GC // QW
    share, halves = rows_k // chans, chans // 2
    cap = 2 * count // planes
    me, time = lax.axis_index("chan"), lax.axis_index("tm")
    half, core = me // 2, me % 2
    code = w_bin[0, :, 0] * tile_count + tile_col[0]
    rows = row_weight[0].reshape(count, halves, 2, share, width_v)
    mine = (vis[0], rows, col_weight[0])
    given = lax.dynamic_slice_in_dim(rows, core ^ 1, 1, 2)
    other = tuple(swap(value, "chan", 1) for value in (vis[0], given, col_weight[0]))
    code_b = swap(code, "chan", 1)
    low = jnp.bfloat16

    codes = jnp.concatenate([code, code_b])

    def grid(ranges, *parts):
        lengths, place = [], jnp.full_like(codes, -1)
        for r, tiles in ranges:
            tile = codes - ((time ^ r) * tile_count + tiles.start)
            inside = (tile >= 0) & (tile < len(tiles))
            place = jnp.where(inside, tile + sum(lengths), place)
            lengths.append(len(tiles))
        meta = jnp.concatenate([jnp.stack([half, core]), place]).astype(jnp.int32)
        return grid_plane(meta, (mine, other), ("hbm", "vmem"), halves, lengths, cap, parts)

    middle, wide = tile_count // 2, jnp.float32
    every = range(tile_count)
    tiles_a, tiles_b = every[:middle], every[middle:]
    half_a, half_b = (0, middle, (wide, low)), (middle, tile_count, (wide, low))
    o3a, s3a, o1b, p1b = grid(
        [(3, tiles_a), (1, tiles_b)], half_a, (middle, tile_count, (low, low))
    )
    o2a, s2a, o2b, s2b = grid([(2, every)], half_a, half_b)
    o3b, s3b, o1a, s1a = grid([(3, tiles_b), (1, tiles_a)], half_a, half_b)
    o0a, s0a, o0b, p0b = grid([(0, every)], half_a, (middle, tile_count, (wide, wide)))

    def give(*values):
        return added(*values).astype(low)

    z1b, z1c = swap(o1b, "tm", 1), swap(p1b, "tm", 1)
    x3a, x3b = swap(s3a, "chan", 2), swap(s3b, "chan", 2)
    x2a, x2b = swap(s2a, "chan", 2), swap(s2b, "chan", 2)
    x1a, x0a = swap(s1a, "chan", 2), swap(s0a, "chan", 2)
    z3a = swap(give(o3a, x3a), "tm", 1)
    z3b = swap(give(o3b, x3b), "tm", 1)
    z2a = swap(give(o2a, x2a, z3a), "tm", 2)
    z2b = swap(give(o2b, x2b, z3b), "tm", 2)
    z1a = swap(give(o1a, x1a), "tm", 1)
    x0b = swap(give(p0b, z1c), "chan", 2)
    out = finish((o0a, x0a, z1a, z2a), w_kernel[0], 0, tile_count)
    out = finish((o0b, z1b, x0b, z2b), w_kernel[0], 1, tile_count, out)
    return out[None]


def body(vis, row_weight, col_weight, w_bin, tile_col, w_kernel):
    planes, chans = lax.axis_size("tm"), lax.axis_size("chan")
    count, _, width_v = vis.shape[1:]
    rows_k, width_q = row_weight.shape[2], col_weight.shape[3]
    dense = planes * (GC // QW) * rows_k * 2 * width_q
    raw = 2 * count * width_v * (rows_k + width_q + 2)
    fits = planes == 4 and chans == 4 and dense <= 2 * raw
    chosen = dense_body if fits else raw_body
    return chosen(vis, row_weight, col_weight, w_bin, tile_col, w_kernel)


def solution(mesh):
    in_specs = (
        P(("groups", "chan"), "tm", None, None),
        P(("groups", "chan"), "tm", None, None),
        P(("groups", "chan"), "tm", None, None),
        P(("groups", "chan"), "tm", None),
        P(("groups", "chan"), "tm"),
        P(("groups", "tm"), None, None),
    )
    out_specs = P(("groups", "tm"), "chan", None, None)
    return jax.shard_map(body, mesh=mesh, in_specs=in_specs, out_specs=out_specs, check_vma=False)
```
